32 devices in a mesh: pop: 8 (over y, x, core), tile: 4 (over z).
Axes of the slice: x: 2, y: 2, z: 4, core: 2. Of those that a mesh axis runs over, the one named last changes fastest.
Arguments:
- weights: int32 [8, 8], replicated, may hold values from -2 to 3
- terminal: float32 [8, 32, 2048], P('pop', 'tile'), may hold values from -4.5 to 4.5
- density_history: bfloat16 [8, 8, 32, 2048], P('pop', None, 'tile'), may hold values from 0.19921875 to 2
- density_init: float32 [8, 32, 2048], P('pop', 'tile'), may hold values from 0.2 to 2
Outputs:
- values: float32 [8, 8, 32, 2048], P('pop', None, 'tile')
- density_final: float32 [8, 32, 2048], P('pop', 'tile')
The draws below stay inside these ranges and needn't reach their ends.
All inputs are finite; a program needn't handle non-finite values.
Results may differ from the reference program's by a relative error of at most 0.0003.
Values may be sent and summed in bfloat16 or wider, within the bound.
A program may use at most 64 MiB of HBM per device.

```python
import math
import jax
import jax.numpy as jnp
from jax import lax

COLS = 2048
STEPS = 8
POPS = 8
ROWS = 32


def draw_terminal(key, part):
    slope_key = jax.random.fold_in(key, 11)
    phase_key = jax.random.fold_in(key, 12)
    noise_key = jax.random.fold_in(key, 13)
    period = 12.0
    phase = jax.random.randint(phase_key, (POPS, 1, 1), 0, 12).astype(jnp.float32)
    rows = jnp.arange(ROWS, dtype=jnp.float32)[None, :, None]
    position = jnp.mod(rows + phase, period)
    ramp = jnp.abs(position - 0.5 * period) - 0.25 * period
    slope = jax.random.uniform(slope_key, (POPS, 1, 1), jnp.float32, 1.0, 1.25)
    noise = 0.2 * jnp.clip(jax.random.normal(noise_key, (POPS, ROWS, COLS), jnp.float32), -3.0, 3.0)
    return slope * ramp + noise


def set_ends(values, own_key, least, largest):
    extent = values.shape
    place = [jax.random.randint(jax.random.fold_in(own_key, axis), (), 0, extent[axis]) for axis in range(len(extent))]
    values = values.at[tuple(place)].set(least)
    longest = extent.index(max(extent))
    place[longest] = (place[longest] + 1) % extent[longest]
    return values.at[tuple(place)].set(largest)


def level_of(key, shape, cuts, least, high):
    loudness = 1.0
    for dim, parts in cuts:
        draws = jax.random.uniform(jax.random.fold_in(jax.random.fold_in(key, 6), dim), (parts,), jnp.float32, least / len(cuts), high / len(cuts))
        loudness = loudness * jnp.repeat(jnp.exp(draws), shape[dim] // parts).reshape((-1,) + (1,) * (len(shape) - 1 - dim))
    return loudness


def setup_inputs(seed: int = 0) -> dict:
    keys = jax.random.split(jax.random.key(seed), 5)
    weights = set_ends(jax.random.randint(keys[0], (POPS, POPS), -2, 4), jax.random.fold_in(keys[0], 1), -2, 3).astype(jnp.int32)
    terminal = draw_terminal(jax.random.fold_in(keys[4], 71), 0)
    density_history = jnp.clip(jnp.exp(math.log(2.0) - 2.306499 * jax.random.uniform(keys[2], (POPS, STEPS, ROWS, COLS), jnp.float32) ** level_of(keys[2], (POPS, STEPS, ROWS, COLS), ((0, 8), (2, 4)), -0.2, 0.2)), 0.19921875, 2.0).astype(jnp.bfloat16)
    density_init = jnp.clip(jnp.exp(math.log(2.0) - 2.3025851 * jax.random.uniform(keys[3], (POPS, ROWS, COLS), jnp.float32) ** level_of(keys[3], (POPS, ROWS, COLS), ((0, 8), (1, 4)), -0.2, 0.2)), 0.2, 2.0)
    return dict(weights=weights, terminal=terminal, density_history=density_history, density_init=density_init)


time_step = 0.2
viscosity = 0.2


def laplace(field):
    return jnp.roll(field, -1, 1) + jnp.roll(field, 1, 1) + jnp.roll(field, -1, 2) + jnp.roll(field, 1, 2) - 4.0 * field


def hamiltonian(field):
    ahead_rows = jnp.minimum(jnp.roll(field, -1, 1) - field, 0.0)
    behind_rows = jnp.maximum(field - jnp.roll(field, 1, 1), 0.0)
    ahead_cols = jnp.minimum(jnp.roll(field, -1, 2) - field, 0.0)
    behind_cols = jnp.maximum(field - jnp.roll(field, 1, 2), 0.0)
    return 0.5 * (behind_rows * behind_rows + ahead_rows * ahead_rows + behind_cols * behind_cols + ahead_cols * ahead_cols)


def transport(density, value):
    drift_rows = -(jnp.roll(value, -1, 1) - value)
    flux_rows = jnp.maximum(drift_rows, 0.0) * density + jnp.minimum(drift_rows, 0.0) * jnp.roll(density, -1, 1)
    drift_cols = -(jnp.roll(value, -1, 2) - value)
    flux_cols = jnp.maximum(drift_cols, 0.0) * density + jnp.minimum(drift_cols, 0.0) * jnp.roll(density, -1, 2)
    div_rows = flux_rows - jnp.roll(flux_rows, 1, 1)
    div_cols = flux_cols - jnp.roll(flux_cols, 1, 2)
    return density + time_step * (viscosity * laplace(density) - div_rows - div_cols)


def reference(weights, terminal, density_history, density_init):
    factors = weights.astype(jnp.float32)
    current = terminal
    centred = [None] * STEPS
    for step in reversed(range(STEPS)):
        coupled = jnp.einsum("pq,qrc->prc", factors, density_history[:, step].astype(jnp.float32), precision=lax.Precision.HIGHEST) / POPS
        advanced = current + time_step * (viscosity * laplace(current) - hamiltonian(current) + coupled)
        advanced = advanced - jnp.mean(advanced, axis=(1, 2), keepdims=True)
        centred[step] = advanced
        current = advanced
    density = density_init
    for step in range(STEPS):
        density = transport(density, centred[step])
    return jnp.stack(centred, axis=1), density
```

```python
import functools

import jax
import jax.numpy as jnp
from jax import lax
from jax.experimental import pallas as pl
from jax.experimental.pallas import tpu as pltpu
from jax.sharding import PartitionSpec as P

time_step = 0.2
viscosity = 0.2
LANES = 128
WINDOWS = 4
SPAN = LANES // WINDOWS
LAG_B, LAG_C, LAG_D = 2, 4, 5


def kernel(pops, tiles, weights, terminal, history, initial, values, density_out,
           gathered, gathered_rim, start_value, start_mass, start_rim,
           rim_send, rim_send_f32, swept, mass_main, slope_r, slope_c, sums_own, sums_all,
           tile_send, tile_recv, tile_self, first_send, first_recv, first_self,
           x_send, x_recv, y_send, y_recv, half_a_send, half_a_recv, half_b_send, half_b_recv,
           core_send, core_recv, back_send, back_recv, back_self):
    steps, rows, cols = history.shape
    width = cols // tiles
    groups = steps // WINDOWS
    total_rows = tiles * rows
    outer = pops // 4
    half = tiles // 2
    me = lax.axis_index("tile")
    own = lax.axis_index("pop")
    core = own % 2
    plane = (own // 2) % 2
    line = own // 4

    def pop_of(a, b, c):
        return (a * 2 + b) * 2 + c

    partner = pop_of(line, plane, 1 - core)
    across = pop_of(line, 1 - plane, core)
    lines = [(line + j) % outer for j in range(1, outer)]
    columns = [pop_of(a, plane, core) for a in lines]
    diagonal = [pop_of(a, 1 - plane, core) for a in lines]
    peers = [(me + d) % tiles for d in range(1, tiles)]

    barrier = pltpu.get_barrier_semaphore()
    greeted = [{"tile": z} for z in peers] + [{"pop": q} for q in [partner, across] + columns]
    for there in greeted:
        pl.semaphore_signal(barrier, inc=1, device_id=there, device_id_type=pl.DeviceIdType.MESH)

    lane = lax.broadcasted_iota(jnp.int32, (rows, LANES), 1)
    window = ((lane + SPAN // 2) % LANES) // SPAN
    right_side = lane < LANES // 2

    def rim_of(block, z):
        right = ((z + 1) % tiles) * width
        left = ((z + tiles - 1) % tiles) * width + width - LANES
        return jnp.where(right_side, block[:, right:right + LANES], block[:, left:left + LANES])

    def packed(parts):
        out = parts[0]
        for k in range(1, len(parts)):
            out = jnp.where(window == k, pltpu.roll(parts[k], SPAN * k, 1), out)
        return out

    for z in range(tiles):
        rim_send_f32[z] = packed([rim_of(terminal[...], z), rim_of(initial[...], z)])
    for g in range(groups):
        for z in range(tiles):
            parts = [rim_of(history[steps - 1 - (g * WINDOWS + k)].astype(jnp.float32), z)
                     for k in range(WINDOWS)]
            rim_send[z, g] = packed(parts).astype(jnp.bfloat16)

    pl.semaphore_wait(barrier, len(greeted))

    def cut(z):
        return pl.ds(pl.multiple_of(z * width, LANES), width)

    sent = []

    def remote(src, dst, send, recv, there):
        copy = pltpu.make_async_remote_copy(src_ref=src, dst_ref=dst, send_sem=send, recv_sem=recv,
                                            device_id=there, device_id_type=pl.DeviceIdType.MESH)
        copy.start()
        return copy

    def arrived(ref, sem):
        pltpu.make_async_copy(ref, ref, sem).wait()

    firsts = [
        (lambda z: terminal.at[:, cut(z)], start_value),
        (lambda z: rim_send_f32.at[z], start_rim),
        (lambda z: initial.at[:, cut(z)], start_mass),
    ]

    def exchange_first(n):
        src, dst = firsts[n]
        pltpu.make_async_copy(src(me), dst.at[me], first_self.at[n]).start()
        for z in peers:
            remote(src(z), dst.at[me], first_send.at[n], first_recv.at[n], {"tile": z})

    def wait_first(n):
        dst = firsts[n][1]
        pltpu.make_async_copy(firsts[n][0](me), dst.at[me], first_self.at[n]).wait()
        arrived(dst.at[pl.ds(0, tiles - 1)], first_recv.at[n])
        arrived(dst.at[pl.ds(0, tiles - 1)], first_send.at[n])

    items = []
    for g in range(groups):
        items.append(("rim", g))
        for k in range(WINDOWS):
            items.append(("main", steps - 1 - (g * WINDOWS + k)))

    def block(n, q):
        kind, index = items[n]
        return gathered.at[q, index] if kind == "main" else gathered_rim.at[q, index]

    def piece(n, z):
        kind, index = items[n]
        return history.at[index, :, cut(z)] if kind == "main" else rim_send.at[z, index]

    def exchange_item(n):
        pltpu.make_async_copy(piece(n, me), block(n, own).at[me], tile_self.at[n]).start()
        for z in peers:
            remote(piece(n, z), block(n, own).at[me], tile_send.at[n], tile_recv.at[n], {"tile": z})

    exchange_item(0)
    exchange_item(1)
    exchange_first(0)
    exchange_first(1)
    for n in range(2, len(items)):
        exchange_item(n)
    exchange_first(2)

    def to_partner(n, kind, q):
        sent.append(remote(block(n, q), block(n, q), core_send.at[kind, n], core_recv.at[kind, n],
                           {"pop": partner}))

    def stage_a(n):
        pltpu.make_async_copy(piece(n, me), block(n, own).at[me], tile_self.at[n]).wait()
        arrived(block(n, own).at[pl.ds(0, tiles - 1)], tile_recv.at[n])
        mine = block(n, own)
        sent.append(remote(mine, mine, x_send.at[n], x_recv.at[n], {"pop": across}))
        for j, q in enumerate(columns):
            sent.append(remote(mine, mine, y_send.at[j, n], y_recv.at[j, n], {"pop": q}))
        to_partner(n, 0, own)

    def part(n, q, which):
        return block(n, q).at[pl.ds(which * half, half)]

    def stage_b(n):
        arrived(block(n, across), x_recv.at[n])
        ref = part(n, across, 1)
        for j, q in enumerate(columns):
            sent.append(remote(ref, ref, half_b_send.at[j, n], half_b_recv.at[j, n], {"pop": q}))
        to_partner(n, 1, across)
        for j in range(outer - 1):
            q = columns[outer - 2 - j]
            arrived(block(n, q), y_recv.at[j, n])
            ref = part(n, q, 0)
            sent.append(remote(ref, ref, half_a_send.at[j, n], half_a_recv.at[j, n], {"pop": across}))
            to_partner(n, 2 + j, q)

    def stage_c(n):
        for j in range(outer - 1):
            q = diagonal[outer - 2 - j]
            arrived(part(n, q, 0), half_a_recv.at[j, n])
            arrived(part(n, q, 1), half_b_recv.at[j, n])
            to_partner(n, 1 + outer + j, q)

    def other(q):
        return q + 1 - 2 * (q % 2)

    def coupled(n):
        for kind in range(2 * outer):
            if kind == 0:
                q = own
            elif kind == 1:
                q = across
            elif kind < 1 + outer:
                q = columns[outer - 2 - (kind - 2)]
            else:
                q = diagonal[outer - 2 - (kind - 1 - outer)]
            arrived(block(n, other(q)), core_recv.at[kind, n])
        total = None
        for q in range(pops):
            factor = weights[own, q].astype(jnp.float32) * (1.0 / pops)
            term = factor * block(n, q)[...].astype(jnp.float32)
            total = term if total is None else total + term
        return total.reshape(total_rows, total.shape[-1])

    full = width + LANES

    def ahead_r(x):
        return pltpu.roll(x, total_rows - 1, 0)

    def behind_r(x):
        return pltpu.roll(x, 1, 0)

    def ahead_c(x):
        return pltpu.roll(x, full - 1, 1)

    def behind_c(x):
        return pltpu.roll(x, 1, 1)

    def rim_at(rim, k):
        return rim if k == 0 else pltpu.roll(rim, LANES - SPAN * k, 1)

    def send_back(src, dst, n):
        pltpu.make_async_copy(src.at[me], dst.at[:, cut(me)], back_self.at[n]).start()
        for z in peers:
            remote(src.at[z], dst.at[:, cut(me)], back_send.at[n], back_recv.at[n], {"tile": z})

    def wait_back(src, dst, n):
        pltpu.make_async_copy(src.at[me], dst.at[:, cut(me)], back_self.at[n]).wait()
        landed = dst.at[:, pl.ds(0, (tiles - 1) * width)]
        arrived(landed, back_recv.at[n])
        arrived(landed, back_send.at[n])

    state = {}

    def stage_d(n):
        kind, t = items[n]
        if n == 0:
            for m in range(2):
                wait_first(m)
            main = start_value[...].reshape(total_rows, width)
            state["u"] = jnp.concatenate([main, start_rim[...].reshape(total_rows, LANES)], axis=1)
        if kind == "rim":
            state["rim"] = coupled(n)
            return
        k = (steps - 1 - t) % WINDOWS
        source = jnp.concatenate([coupled(n), rim_at(state["rim"], k)], axis=1)
        u = state["u"]
        dr = ahead_r(u) - u
        dc = ahead_c(u) - u
        if t + 1 < steps:
            slope_r[t + 1] = dr
            slope_c[t + 1] = dc
        er, ec = behind_r(dr), behind_c(dc)
        br, bc = jnp.maximum(er, 0.0), jnp.maximum(ec, 0.0)
        ar, ac = jnp.minimum(dr, 0.0), jnp.minimum(dc, 0.0)
        lap = (dr - er) + (dc - ec)
        ham = 0.5 * ((br * br + ar * ar) + (bc * bc + ac * ac))
        u = u + time_step * (viscosity * lap - ham + source)
        state["u"] = u
        main = u[:, :width]
        swept[t] = main.reshape(tiles, rows, width)
        send_back(swept.at[t], values.at[t], t)
        line_sum = jnp.sum(main, axis=0, keepdims=True)
        folded = line_sum[:, :LANES]
        for j in range(1, width // LANES):
            folded = folded + line_sum[:, j * LANES:(j + 1) * LANES]
        sums_own[t:t + 1, :] = folded

    count = len(items)
    for i in range(count + LAG_D):
        if i < count:
            stage_a(i)
        if 0 <= i - LAG_B < count:
            stage_b(i - LAG_B)
        if 0 <= i - LAG_C < count:
            stage_c(i - LAG_C)
        if 0 <= i - LAG_D < count:
            stage_d(i - LAG_D)

    sums_n = steps + 1
    sums_all[me] = sums_own[...]
    for z in peers:
        remote(sums_own, sums_all.at[me], back_send.at[sums_n], back_recv.at[sums_n], {"tile": z})

    wait_first(2)
    u = state["u"]
    mass = jnp.concatenate([start_mass[...].reshape(total_rows, width),
                            rim_at(start_rim[...].reshape(total_rows, LANES), 1)], axis=1)
    for t in range(steps):
        if t == 0:
            dr, dc = ahead_r(u) - u, ahead_c(u) - u
        else:
            dr, dc = slope_r[t], slope_c[t]
        mr, mc = ahead_r(mass), ahead_c(mass)
        flux_r = jnp.maximum(-dr, 0.0) * mass + jnp.minimum(-dr, 0.0) * mr
        flux_c = jnp.maximum(-dc, 0.0) * mass + jnp.minimum(-dc, 0.0) * mc
        net_r = viscosity * (mr - mass) - flux_r
        net_c = viscosity * (mc - mass) - flux_c
        mass = mass + time_step * ((net_r - behind_r(net_r)) + (net_c - behind_c(net_c)))
    mass_main[...] = mass[:, :width].reshape(tiles, rows, width)
    send_back(mass_main, density_out, steps)

    arrived(sums_all.at[pl.ds(0, tiles - 1)], back_recv.at[sums_n])
    arrived(sums_all.at[pl.ds(0, tiles - 1)], back_send.at[sums_n])
    grand = jnp.sum(jnp.sum(sums_all[...], axis=0), axis=1, keepdims=True) * (1.0 / (total_rows * cols))
    for t in reversed(range(steps)):
        wait_back(swept.at[t], values.at[t], t)
        values[t] = values[t] - grand[t:t + 1, :]
    wait_back(mass_main, density_out, steps)
    for n in range(count):
        arrived(block(n, own).at[pl.ds(0, tiles - 1)], tile_send.at[n])
    for copy in sent:
        copy.wait_send()


def per_device(pops, tiles, weights, terminal, density_history, density_init):
    _, steps, rows, cols = density_history.shape
    width = cols // tiles
    groups = steps // WINDOWS
    items = steps + groups
    outer = pops // 4
    total_rows = tiles * rows
    full = width + LANES
    dma = pltpu.SemaphoreType.DMA
    lines = max(outer - 1, 1)
    vmem = pl.BlockSpec(memory_space=pltpu.VMEM)
    values, density = pl.pallas_call(
        functools.partial(kernel, pops, tiles),
        out_shape=(
            jax.ShapeDtypeStruct((steps, rows, cols), jnp.float32),
            jax.ShapeDtypeStruct((rows, cols), jnp.float32),
        ),
        in_specs=[pl.BlockSpec(memory_space=pltpu.SMEM), vmem, vmem, vmem],
        out_specs=(vmem, vmem),
        scratch_shapes=[
            pltpu.VMEM((pops, steps, tiles, rows, width), jnp.bfloat16),
            pltpu.VMEM((pops, groups, tiles, rows, LANES), jnp.bfloat16),
            pltpu.VMEM((tiles, rows, width), jnp.float32),
            pltpu.VMEM((tiles, rows, width), jnp.float32),
            pltpu.VMEM((tiles, rows, LANES), jnp.float32),
            pltpu.VMEM((tiles, groups, rows, LANES), jnp.bfloat16),
            pltpu.VMEM((tiles, rows, LANES), jnp.float32),
            pltpu.VMEM((steps, tiles, rows, width), jnp.float32),
            pltpu.VMEM((tiles, rows, width), jnp.float32),
            pltpu.VMEM((steps, total_rows, full), jnp.float32),
            pltpu.VMEM((steps, total_rows, full), jnp.float32),
            pltpu.VMEM((steps, LANES), jnp.float32),
            pltpu.VMEM((tiles, steps, LANES), jnp.float32),
            dma((items,)), dma((items,)), dma((items,)),
            dma((3,)), dma((3,)), dma((3,)),
            dma((items,)), dma((items,)),
            dma((lines, items)), dma((lines, items)),
            dma((lines, items)), dma((lines, items)),
            dma((lines, items)), dma((lines, items)),
            dma((2 * outer, items)), dma((2 * outer, items)),
            dma((steps + 2,)), dma((steps + 2,)), dma((steps + 1,)),
        ],
        compiler_params=pltpu.CompilerParams(collective_id=0, has_side_effects=True),
    )(weights, terminal[0], density_history[0], density_init[0])
    return values[None], density[None]


def solution(mesh):
    in_specs = (P(), P("pop", "tile", None), P("pop", None, "tile", None), P("pop", "tile", None))
    out_specs = (P("pop", None, "tile", None), P("pop", "tile", None))
    body = functools.partial(per_device, mesh.shape["pop"], mesh.shape["tile"])
    return jax.shard_map(body, mesh=mesh, in_specs=in_specs, out_specs=out_specs, check_vma=False)
```

```python
import functools

import jax
import jax.numpy as jnp
from jax import lax
from jax.experimental import pallas as pl
from jax.experimental.pallas import tpu as pltpu
from jax.sharding import PartitionSpec as P

time_step = 0.2
viscosity = 0.2
LANES = 128
WINDOWS = 4
SPAN = LANES // WINDOWS
LAG_B, LAG_C, LAG_D = 3, 3, 4
DIRECT = 10


def kernel(pops, tiles, weights, terminal_in, history_in, initial_in, values, density_out,
           terminal, history, initial, load_sem, gathered, gathered_rim, start_value, start_mass, start_rim,
           rim_send, rim_send_f32, swept, mass_main, slope_r, slope_c, sums_own, sums_all,
           tile_send, tile_recv, tile_self, first_send, first_recv, first_self,
           x_send, x_recv, y_send, y_recv, half_a_send, half_a_recv, half_b_send, half_b_recv,
           core_send, core_recv, back_send, back_recv, back_self):
    steps, rows, cols = history.shape
    width = cols // tiles
    groups = steps // WINDOWS
    total_rows = tiles * rows
    outer = pops // 4
    half = tiles // 2
    me = lax.axis_index("tile")
    own = lax.axis_index("pop")
    core = own % 2
    plane = (own // 2) % 2
    line = own // 4

    def pop_of(a, b, c):
        return (a * 2 + b) * 2 + c

    partner = pop_of(line, plane, 1 - core)
    across = pop_of(line, 1 - plane, core)
    lines = [(line + j) % outer for j in range(1, outer)]
    columns = [pop_of(a, plane, core) for a in lines]
    diagonal = [pop_of(a, 1 - plane, core) for a in lines]
    peers = [(me + d) % tiles for d in range(1, tiles)]

    barrier = pltpu.get_barrier_semaphore()
    greeted = [{"tile": z} for z in peers] + [{"pop": q} for q in [partner, across] + columns + diagonal]
    for there in greeted:
        pl.semaphore_signal(barrier, inc=1, device_id=there, device_id_type=pl.DeviceIdType.MESH)

    loads = [pltpu.make_async_copy(src, dst, load_sem.at[n]) for n, (src, dst) in enumerate(
        [(terminal_in, terminal), (initial_in, initial), (history_in, history)])]
    for load in loads:
        load.start()
    for load in loads:
        load.wait()
    lane = lax.broadcasted_iota(jnp.int32, (rows, LANES), 1)
    window = ((lane + SPAN // 2) % LANES) // SPAN
    right_side = lane < LANES // 2

    def rim_of(block, z):
        right = ((z + 1) % tiles) * width
        left = ((z + tiles - 1) % tiles) * width + width - LANES
        return jnp.where(right_side, block[:, right:right + LANES], block[:, left:left + LANES])

    def packed(parts):
        out = parts[0]
        for k in range(1, len(parts)):
            out = jnp.where(window == k, pltpu.roll(parts[k], SPAN * k, 1), out)
        return out

    for z in range(tiles):
        rim_send_f32[z] = packed([rim_of(terminal[...], z), rim_of(initial[...], z)])
    for g in range(groups):
        for z in range(tiles):
            parts = [rim_of(history[steps - 1 - (g * WINDOWS + k)].astype(jnp.float32), z)
                     for k in range(WINDOWS)]
            rim_send[z, g] = packed(parts).astype(jnp.bfloat16)

    pl.semaphore_wait(barrier, len(greeted))

    def cut(z):
        return pl.ds(pl.multiple_of(z * width, LANES), width)

    sent = []

    def remote(src, dst, send, recv, there):
        copy = pltpu.make_async_remote_copy(src_ref=src, dst_ref=dst, send_sem=send, recv_sem=recv,
                                            device_id=there, device_id_type=pl.DeviceIdType.MESH)
        copy.start()
        return copy

    def arrived(ref, sem):
        pltpu.make_async_copy(ref, ref, sem).wait()

    firsts = [
        (lambda z: terminal.at[:, cut(z)], start_value),
        (lambda z: rim_send_f32.at[z], start_rim),
        (lambda z: initial.at[:, cut(z)], start_mass),
    ]

    def exchange_first(n):
        src, dst = firsts[n]
        pltpu.make_async_copy(src(me), dst.at[me], first_self.at[n]).start()
        for z in peers:
            remote(src(z), dst.at[me], first_send.at[n], first_recv.at[n], {"tile": z})

    def wait_first(n):
        dst = firsts[n][1]
        pltpu.make_async_copy(firsts[n][0](me), dst.at[me], first_self.at[n]).wait()
        arrived(dst.at[pl.ds(0, tiles - 1)], first_recv.at[n])
        arrived(dst.at[pl.ds(0, tiles - 1)], first_send.at[n])

    items = []
    for g in range(groups):
        items.append(("rim", g))
        for k in range(WINDOWS):
            items.append(("main", steps - 1 - (g * WINDOWS + k)))

    def block(n, q):
        kind, index = items[n]
        return gathered.at[q, index] if kind == "main" else gathered_rim.at[q, index]

    def piece(n, z):
        kind, index = items[n]
        return history.at[index, :, cut(z)] if kind == "main" else rim_send.at[z, index]

    def exchange_item(n):
        pltpu.make_async_copy(piece(n, me), block(n, own).at[me], tile_self.at[n]).start()
        for z in peers:
            remote(piece(n, z), block(n, own).at[me], tile_send.at[n], tile_recv.at[n], {"tile": z})

    exchange_item(0)
    exchange_item(1)
    exchange_first(0)
    exchange_first(1)
    for n in range(2, len(items)):
        exchange_item(n)
    exchange_first(2)

    def to_partner(n, kind, q):
        sent.append(remote(block(n, q), block(n, q), core_send.at[kind, n], core_recv.at[kind, n],
                           {"pop": partner}))

    def direct(n):
        return n >= len(items) - DIRECT

    def stage_a(n):
        pltpu.make_async_copy(piece(n, me), block(n, own).at[me], tile_self.at[n]).wait()
        arrived(block(n, own).at[pl.ds(0, tiles - 1)], tile_recv.at[n])
        mine = block(n, own)
        sent.append(remote(mine, mine, x_send.at[n], x_recv.at[n], {"pop": across}))
        for j, q in enumerate(columns):
            sent.append(remote(mine, mine, y_send.at[j, n], y_recv.at[j, n], {"pop": q}))
        if direct(n):
            for j, q in enumerate(diagonal):
                sent.append(remote(mine, mine, half_a_send.at[j, n], half_a_recv.at[j, n], {"pop": q}))
        to_partner(n, 0, own)

    def part(n, q, which):
        return block(n, q).at[pl.ds(which * half, half)]

    def stage_b(n):
        arrived(block(n, across), x_recv.at[n])
        ref = part(n, across, 1)
        for j, q in enumerate([] if direct(n) else columns):
            sent.append(remote(ref, ref, half_b_send.at[j, n], half_b_recv.at[j, n], {"pop": q}))
        to_partner(n, 1, across)
        for j in range(outer - 1):
            q = columns[outer - 2 - j]
            arrived(block(n, q), y_recv.at[j, n])
            ref = part(n, q, 0)
            if not direct(n):
                sent.append(remote(ref, ref, half_a_send.at[j, n], half_a_recv.at[j, n], {"pop": across}))
            to_partner(n, 2 + j, q)

    def stage_c(n):
        for j in range(outer - 1):
            q = diagonal[outer - 2 - j]
            if direct(n):
                arrived(block(n, q), half_a_recv.at[j, n])
            else:
                arrived(part(n, q, 0), half_a_recv.at[j, n])
                arrived(part(n, q, 1), half_b_recv.at[j, n])
            to_partner(n, 1 + outer + j, q)

    def other(q):
        return q + 1 - 2 * (q % 2)

    def coupled(n):
        for kind in range(2 * outer):
            if kind == 0:
                q = own
            elif kind == 1:
                q = across
            elif kind < 1 + outer:
                q = columns[outer - 2 - (kind - 2)]
            else:
                q = diagonal[outer - 2 - (kind - 1 - outer)]
            arrived(block(n, other(q)), core_recv.at[kind, n])
        total = None
        for q in range(pops):
            factor = weights[own, q].astype(jnp.float32) * (1.0 / pops)
            term = factor * block(n, q)[...].astype(jnp.float32)
            total = term if total is None else total + term
        return total.reshape(total_rows, total.shape[-1])

    full = width + LANES

    def ahead_r(x):
        return pltpu.roll(x, total_rows - 1, 0)

    def behind_r(x):
        return pltpu.roll(x, 1, 0)

    def ahead_c(x):
        return pltpu.roll(x, full - 1, 1)

    def behind_c(x):
        return pltpu.roll(x, 1, 1)

    def rim_at(rim, k):
        return rim if k == 0 else pltpu.roll(rim, LANES - SPAN * k, 1)

    def send_back(src, dst, n):
        pltpu.make_async_copy(src.at[me], dst.at[:, cut(me)], back_self.at[n]).start()
        for z in peers:
            remote(src.at[z], dst.at[:, cut(me)], back_send.at[n], back_recv.at[n], {"tile": z})

    def wait_back(src, dst, n):
        pltpu.make_async_copy(src.at[me], dst.at[:, cut(me)], back_self.at[n]).wait()
        landed = dst.at[:, pl.ds(0, (tiles - 1) * width)]
        arrived(landed, back_recv.at[n])
        arrived(landed, back_send.at[n])

    state = {}

    def stage_d(n):
        kind, t = items[n]
        if n == 0:
            for m in range(2):
                wait_first(m)
            main = start_value[...].reshape(total_rows, width)
            state["u"] = jnp.concatenate([main, start_rim[...].reshape(total_rows, LANES)], axis=1)
        if kind == "rim":
            state["rim"] = coupled(n)
            return
        k = (steps - 1 - t) % WINDOWS
        source = jnp.concatenate([coupled(n), rim_at(state["rim"], k)], axis=1)
        u = state["u"]
        dr = ahead_r(u) - u
        dc = ahead_c(u) - u
        if t + 1 < steps:
            slope_r[t + 1] = dr
            slope_c[t + 1] = dc
        er, ec = behind_r(dr), behind_c(dc)
        br, bc = jnp.maximum(er, 0.0), jnp.maximum(ec, 0.0)
        ar, ac = jnp.minimum(dr, 0.0), jnp.minimum(dc, 0.0)
        lap = (dr - er) + (dc - ec)
        ham = 0.5 * ((br * br + ar * ar) + (bc * bc + ac * ac))
        u = u + time_step * (viscosity * lap - ham + source)
        state["u"] = u
        main = u[:, :width]
        swept[t] = main.reshape(tiles, rows, width)
        send_back(swept.at[t], values.at[t], t)
        line_sum = jnp.sum(main, axis=0, keepdims=True)
        folded = line_sum[:, :LANES]
        for j in range(1, width // LANES):
            folded = folded + line_sum[:, j * LANES:(j + 1) * LANES]
        sums_own[t:t + 1, :] = folded

    count = len(items)
    for i in range(count + LAG_D):
        if i < count:
            stage_a(i)
        if 0 <= i - LAG_B < count:
            stage_b(i - LAG_B)
        if 0 <= i - LAG_C < count:
            stage_c(i - LAG_C)
        if 0 <= i - LAG_D < count:
            stage_d(i - LAG_D)

    sums_n = steps + 1
    sums_all[me] = sums_own[...]
    for z in peers:
        remote(sums_own, sums_all.at[me], back_send.at[sums_n], back_recv.at[sums_n], {"tile": z})

    wait_first(2)
    u = state["u"]
    mass = jnp.concatenate([start_mass[...].reshape(total_rows, width),
                            rim_at(start_rim[...].reshape(total_rows, LANES), 1)], axis=1)
    for t in range(steps):
        if t == 0:
            dr, dc = ahead_r(u) - u, ahead_c(u) - u
        else:
            dr, dc = slope_r[t], slope_c[t]
        mr, mc = ahead_r(mass), ahead_c(mass)
        flux_r = jnp.maximum(-dr, 0.0) * mass + jnp.minimum(-dr, 0.0) * mr
        flux_c = jnp.maximum(-dc, 0.0) * mass + jnp.minimum(-dc, 0.0) * mc
        net_r = viscosity * (mr - mass) - flux_r
        net_c = viscosity * (mc - mass) - flux_c
        mass = mass + time_step * ((net_r - behind_r(net_r)) + (net_c - behind_c(net_c)))
    mass_main[...] = mass[:, :width].reshape(tiles, rows, width)
    send_back(mass_main, density_out, steps)

    arrived(sums_all.at[pl.ds(0, tiles - 1)], back_recv.at[sums_n])
    arrived(sums_all.at[pl.ds(0, tiles - 1)], back_send.at[sums_n])
    grand = jnp.sum(jnp.sum(sums_all[...], axis=0), axis=1, keepdims=True) * (1.0 / (total_rows * cols))
    for t in reversed(range(steps)):
        wait_back(swept.at[t], values.at[t], t)
        values[t] = values[t] - grand[t:t + 1, :]
    wait_back(mass_main, density_out, steps)
    for n in range(count):
        arrived(block(n, own).at[pl.ds(0, tiles - 1)], tile_send.at[n])
    for copy in sent:
        copy.wait_send()


def finish(values, density, values_out, density_out, sems):
    copies = [
        pltpu.make_async_copy(values, values_out, sems.at[0]),
        pltpu.make_async_copy(density, density_out, sems.at[1]),
    ]
    for copy in copies:
        copy.start()
    for copy in copies:
        copy.wait()


def per_device(pops, tiles, weights, terminal, density_history, density_init):
    _, steps, rows, cols = density_history.shape
    width = cols // tiles
    groups = steps // WINDOWS
    items = steps + groups
    outer = pops // 4
    total_rows = tiles * rows
    full = width + LANES
    dma = pltpu.SemaphoreType.DMA
    lines = max(outer - 1, 1)
    vmem = pl.BlockSpec(memory_space=pltpu.VMEM)
    anywhere = pl.BlockSpec(memory_space=pl.ANY)
    values, density = pl.pallas_call(
        functools.partial(kernel, pops, tiles),
        out_shape=(
            pltpu.VMEM((steps, rows, cols), jnp.float32),
            pltpu.VMEM((rows, cols), jnp.float32),
        ),
        in_specs=[pl.BlockSpec(memory_space=pltpu.SMEM), anywhere, anywhere, anywhere],
        out_specs=(vmem, vmem),
        scratch_shapes=[
            pltpu.VMEM((rows, cols), jnp.float32),
            pltpu.VMEM((steps, rows, cols), jnp.bfloat16),
            pltpu.VMEM((rows, cols), jnp.float32),
            dma((3,)),
            pltpu.VMEM((pops, steps, tiles, rows, width), jnp.bfloat16),
            pltpu.VMEM((pops, groups, tiles, rows, LANES), jnp.bfloat16),
            pltpu.VMEM((tiles, rows, width), jnp.float32),
            pltpu.VMEM((tiles, rows, width), jnp.float32),
            pltpu.VMEM((tiles, rows, LANES), jnp.float32),
            pltpu.VMEM((tiles, groups, rows, LANES), jnp.bfloat16),
            pltpu.VMEM((tiles, rows, LANES), jnp.float32),
            pltpu.VMEM((steps, tiles, rows, width), jnp.float32),
            pltpu.VMEM((tiles, rows, width), jnp.float32),
            pltpu.VMEM((steps, total_rows, full), jnp.float32),
            pltpu.VMEM((steps, total_rows, full), jnp.float32),
            pltpu.VMEM((steps, LANES), jnp.float32),
            pltpu.VMEM((tiles, steps, LANES), jnp.float32),
            dma((items,)), dma((items,)), dma((items,)),
            dma((3,)), dma((3,)), dma((3,)),
            dma((items,)), dma((items,)),
            dma((lines, items)), dma((lines, items)),
            dma((lines, items)), dma((lines, items)),
            dma((lines, items)), dma((lines, items)),
            dma((2 * outer, items)), dma((2 * outer, items)),
            dma((steps + 2,)), dma((steps + 2,)), dma((steps + 1,)),
        ],
        compiler_params=pltpu.CompilerParams(collective_id=0, has_side_effects=True),
    )(weights, terminal[0], density_history[0], density_init[0])
    values, density = pl.pallas_call(
        finish,
        out_shape=(
            jax.ShapeDtypeStruct((steps, rows, cols), jnp.float32),
            jax.ShapeDtypeStruct((rows, cols), jnp.float32),
        ),
        in_specs=[anywhere, anywhere],
        out_specs=(anywhere, anywhere),
        scratch_shapes=[dma((2,))],
        compiler_params=pltpu.CompilerParams(vmem_limit_bytes=8 * 1024 * 1024),
    )(values, density)
    return values[None], density[None]


def solution(mesh):
    in_specs = (P(), P("pop", "tile", None), P("pop", None, "tile", None), P("pop", "tile", None))
    out_specs = (P("pop", None, "tile", None), P("pop", "tile", None))
    body = functools.partial(per_device, mesh.shape["pop"], mesh.shape["tile"])
    return jax.shard_map(body, mesh=mesh, in_specs=in_specs, out_specs=out_specs, check_vma=False)
```

```python
import functools

import jax
import jax.numpy as jnp
from jax import lax
from jax.experimental import pallas as pl
from jax.experimental.pallas import tpu as pltpu
from jax.sharding import PartitionSpec as P

time_step = 0.2
viscosity = 0.2
LANES = 128
WINDOWS = 4
SPAN = LANES // WINDOWS
LAG_B, LAG_C, LAG_D = 3, 3, 4
DIRECT = 10
TWIN = 1


def kernel(pops, tiles, weights, terminal_in, history_in, initial_in, values, density_out,
           terminal, history, initial, load_sem, gathered, gathered_rim, start_value, start_mass, start_rim,
           rim_send, rim_send_f32, swept, mass_main, slope_r, slope_c, sums_own, sums_all,
           tile_send, tile_recv, tile_self, first_send, first_recv, first_self,
           x_send, x_recv, y_send, y_recv, half_a_send, half_a_recv, half_b_send, half_b_recv,
           core_send, core_recv, back_send, back_recv, back_self):
    steps, rows, cols = history.shape
    width = cols // tiles
    groups = steps // WINDOWS
    total_rows = tiles * rows
    outer = pops // 4
    half = tiles // 2
    me = lax.axis_index("tile")
    own = lax.axis_index("pop")
    core = own % 2
    plane = (own // 2) % 2
    line = own // 4

    def pop_of(a, b, c):
        return (a * 2 + b) * 2 + c

    partner = pop_of(line, plane, 1 - core)
    across = pop_of(line, 1 - plane, core)
    lines = [(line + j) % outer for j in range(1, outer)]
    columns = [pop_of(a, plane, core) for a in lines]
    diagonal = [pop_of(a, 1 - plane, core) for a in lines]
    peers = [(me + d) % tiles for d in range(1, tiles)]

    barrier = pltpu.get_barrier_semaphore()
    far = [across] + columns + diagonal
    far_twin = [q + 1 - 2 * (q % 2) for q in far]
    greeted = [{"tile": z} for z in peers] + [{"pop": q} for q in [partner] + far + far_twin]
    for there in greeted:
        pl.semaphore_signal(barrier, inc=1, device_id=there, device_id_type=pl.DeviceIdType.MESH)

    loads = [pltpu.make_async_copy(src, dst, load_sem.at[n]) for n, (src, dst) in enumerate(
        [(terminal_in, terminal), (initial_in, initial), (history_in, history)])]
    for load in loads:
        load.start()
    for load in loads:
        load.wait()
    lane = lax.broadcasted_iota(jnp.int32, (rows, LANES), 1)
    window = ((lane + SPAN // 2) % LANES) // SPAN
    right_side = lane < LANES // 2

    def rim_of(block, z):
        right = ((z + 1) % tiles) * width
        left = ((z + tiles - 1) % tiles) * width + width - LANES
        return jnp.where(right_side, block[:, right:right + LANES], block[:, left:left + LANES])

    def packed(parts):
        out = parts[0]
        for k in range(1, len(parts)):
            out = jnp.where(window == k, pltpu.roll(parts[k], SPAN * k, 1), out)
        return out

    for z in range(tiles):
        rim_send_f32[z] = packed([rim_of(terminal[...], z), rim_of(initial[...], z)])
    for g in range(groups):
        for z in range(tiles):
            parts = [rim_of(history[steps - 1 - (g * WINDOWS + k)].astype(jnp.float32), z)
                     for k in range(WINDOWS)]
            rim_send[z, g] = packed(parts).astype(jnp.bfloat16)

    pl.semaphore_wait(barrier, len(greeted))

    def cut(z):
        return pl.ds(pl.multiple_of(z * width, LANES), width)

    sent = []

    def remote(src, dst, send, recv, there):
        copy = pltpu.make_async_remote_copy(src_ref=src, dst_ref=dst, send_sem=send, recv_sem=recv,
                                            device_id=there, device_id_type=pl.DeviceIdType.MESH)
        copy.start()
        return copy

    def arrived(ref, sem):
        pltpu.make_async_copy(ref, ref, sem).wait()

    firsts = [
        (lambda z: terminal.at[:, cut(z)], start_value),
        (lambda z: rim_send_f32.at[z], start_rim),
        (lambda z: initial.at[:, cut(z)], start_mass),
    ]

    def exchange_first(n):
        src, dst = firsts[n]
        pltpu.make_async_copy(src(me), dst.at[me], first_self.at[n]).start()
        for z in peers:
            remote(src(z), dst.at[me], first_send.at[n], first_recv.at[n], {"tile": z})

    def wait_first(n):
        dst = firsts[n][1]
        pltpu.make_async_copy(firsts[n][0](me), dst.at[me], first_self.at[n]).wait()
        arrived(dst.at[pl.ds(0, tiles - 1)], first_recv.at[n])
        arrived(dst.at[pl.ds(0, tiles - 1)], first_send.at[n])

    items = []
    for g in range(groups):
        items.append(("rim", g))
        for k in range(WINDOWS):
            items.append(("main", steps - 1 - (g * WINDOWS + k)))

    def block(n, q):
        kind, index = items[n]
        return gathered.at[q, index] if kind == "main" else gathered_rim.at[q, index]

    def piece(n, z):
        kind, index = items[n]
        return history.at[index, :, cut(z)] if kind == "main" else rim_send.at[z, index]

    def exchange_item(n):
        pltpu.make_async_copy(piece(n, me), block(n, own).at[me], tile_self.at[n]).start()
        for z in peers:
            remote(piece(n, z), block(n, own).at[me], tile_send.at[n], tile_recv.at[n], {"tile": z})

    exchange_item(0)
    exchange_item(1)
    exchange_first(0)
    exchange_first(1)
    for n in range(2, len(items)):
        exchange_item(n)
    exchange_first(2)

    def to_partner(n, kind, q):
        sent.append(remote(block(n, q), block(n, q), core_send.at[kind, n], core_recv.at[kind, n],
                           {"pop": partner}))

    def direct(n):
        return n >= len(items) - DIRECT

    def twin(n):
        return n >= len(items) - TWIN

    def twin_slot(kind):
        return kind

    def stage_a(n):
        pltpu.make_async_copy(piece(n, me), block(n, own).at[me], tile_self.at[n]).wait()
        arrived(block(n, own).at[pl.ds(0, tiles - 1)], tile_recv.at[n])
        mine = block(n, own)
        sent.append(remote(mine, mine, x_send.at[n], x_recv.at[n], {"pop": across}))
        for j, q in enumerate(columns):
            sent.append(remote(mine, mine, y_send.at[j, n], y_recv.at[j, n], {"pop": q}))
        if direct(n):
            for j, q in enumerate(diagonal):
                sent.append(remote(mine, mine, half_a_send.at[j, n], half_a_recv.at[j, n], {"pop": q}))
        if twin(n):
            for kind, q in enumerate(far_twin):
                sent.append(remote(mine, mine, core_send.at[kind + 1, n], core_recv.at[twin_slot(kind + 1), n], {"pop": q}))
        to_partner(n, 0, own)

    def part(n, q, which):
        return block(n, q).at[pl.ds(which * half, half)]

    def stage_b(n):
        arrived(block(n, across), x_recv.at[n])
        ref = part(n, across, 1)
        for j, q in enumerate([] if direct(n) else columns):
            sent.append(remote(ref, ref, half_b_send.at[j, n], half_b_recv.at[j, n], {"pop": q}))
        if not twin(n):
            to_partner(n, 1, across)
        for j in range(outer - 1):
            q = columns[outer - 2 - j]
            arrived(block(n, q), y_recv.at[j, n])
            ref = part(n, q, 0)
            if not direct(n):
                sent.append(remote(ref, ref, half_a_send.at[j, n], half_a_recv.at[j, n], {"pop": across}))
            if not twin(n):
                to_partner(n, 2 + j, q)

    def stage_c(n):
        for j in range(outer - 1):
            q = diagonal[outer - 2 - j]
            if direct(n):
                arrived(block(n, q), half_a_recv.at[j, n])
            else:
                arrived(part(n, q, 0), half_a_recv.at[j, n])
                arrived(part(n, q, 1), half_b_recv.at[j, n])
            if not twin(n):
                to_partner(n, 1 + outer + j, q)

    def other(q):
        return q + 1 - 2 * (q % 2)

    def coupled(n):
        for kind in range(2 * outer):
            if kind == 0:
                q = own
            elif kind == 1:
                q = across
            elif kind < 1 + outer:
                q = columns[outer - 2 - (kind - 2)]
            else:
                q = diagonal[outer - 2 - (kind - 1 - outer)]
            arrived(block(n, other(q)), core_recv.at[kind, n])
        total = None
        for q in range(pops):
            factor = weights[own, q].astype(jnp.float32) * (1.0 / pops)
            term = factor * block(n, q)[...].astype(jnp.float32)
            total = term if total is None else total + term
        return total.reshape(total_rows, total.shape[-1])

    full = width + LANES

    def ahead_r(x):
        return pltpu.roll(x, total_rows - 1, 0)

    def behind_r(x):
        return pltpu.roll(x, 1, 0)

    def ahead_c(x):
        return pltpu.roll(x, full - 1, 1)

    def behind_c(x):
        return pltpu.roll(x, 1, 1)

    def rim_at(rim, k):
        return rim if k == 0 else pltpu.roll(rim, LANES - SPAN * k, 1)

    def send_back(src, dst, n):
        pltpu.make_async_copy(src.at[me], dst.at[:, cut(me)], back_self.at[n]).start()
        for z in peers:
            remote(src.at[z], dst.at[:, cut(me)], back_send.at[n], back_recv.at[n], {"tile": z})

    def wait_back(src, dst, n):
        pltpu.make_async_copy(src.at[me], dst.at[:, cut(me)], back_self.at[n]).wait()
        landed = dst.at[:, pl.ds(0, (tiles - 1) * width)]
        arrived(landed, back_recv.at[n])
        arrived(landed, back_send.at[n])

    state = {}

    def stage_d(n):
        kind, t = items[n]
        if n == 0:
            for m in range(2):
                wait_first(m)
            main = start_value[...].reshape(total_rows, width)
            state["u"] = jnp.concatenate([main, start_rim[...].reshape(total_rows, LANES)], axis=1)
        if kind == "rim":
            state["rim"] = coupled(n)
            return
        k = (steps - 1 - t) % WINDOWS
        source = jnp.concatenate([coupled(n), rim_at(state["rim"], k)], axis=1)
        u = state["u"]
        dr = ahead_r(u) - u
        dc = ahead_c(u) - u
        if t + 1 < steps:
            slope_r[t + 1] = dr
            slope_c[t + 1] = dc
        er, ec = behind_r(dr), behind_c(dc)
        br, bc = jnp.maximum(er, 0.0), jnp.maximum(ec, 0.0)
        ar, ac = jnp.minimum(dr, 0.0), jnp.minimum(dc, 0.0)
        lap = (dr - er) + (dc - ec)
        ham = 0.5 * ((br * br + ar * ar) + (bc * bc + ac * ac))
        u = u + time_step * (viscosity * lap - ham + source)
        state["u"] = u
        main = u[:, :width]
        swept[t] = main.reshape(tiles, rows, width)
        send_back(swept.at[t], values.at[t], t)
        line_sum = jnp.sum(main, axis=0, keepdims=True)
        folded = line_sum[:, :LANES]
        for j in range(1, width // LANES):
            folded = folded + line_sum[:, j * LANES:(j + 1) * LANES]
        sums_own[t:t + 1, :] = folded

    count = len(items)
    for i in range(count + LAG_D):
        if i < count:
            stage_a(i)
        if 0 <= i - LAG_B < count:
            stage_b(i - LAG_B)
        if 0 <= i - LAG_C < count:
            stage_c(i - LAG_C)
        if 0 <= i - LAG_D < count:
            stage_d(i - LAG_D)

    sums_n = steps + 1
    sums_all[me] = sums_own[...]
    for z in peers:
        remote(sums_own, sums_all.at[me], back_send.at[sums_n], back_recv.at[sums_n], {"tile": z})

    wait_first(2)
    u = state["u"]
    mass = jnp.concatenate([start_mass[...].reshape(total_rows, width),
                            rim_at(start_rim[...].reshape(total_rows, LANES), 1)], axis=1)
    for t in range(steps):
        if t == 0:
            dr, dc = ahead_r(u) - u, ahead_c(u) - u
        else:
            dr, dc = slope_r[t], slope_c[t]
        mr, mc = ahead_r(mass), ahead_c(mass)
        flux_r = jnp.maximum(-dr, 0.0) * mass + jnp.minimum(-dr, 0.0) * mr
        flux_c = jnp.maximum(-dc, 0.0) * mass + jnp.minimum(-dc, 0.0) * mc
        net_r = viscosity * (mr - mass) - flux_r
        net_c = viscosity * (mc - mass) - flux_c
        mass = mass + time_step * ((net_r - behind_r(net_r)) + (net_c - behind_c(net_c)))
    mass_main[...] = mass[:, :width].reshape(tiles, rows, width)
    send_back(mass_main, density_out, steps)

    arrived(sums_all.at[pl.ds(0, tiles - 1)], back_recv.at[sums_n])
    arrived(sums_all.at[pl.ds(0, tiles - 1)], back_send.at[sums_n])
    grand = jnp.sum(jnp.sum(sums_all[...], axis=0), axis=1, keepdims=True) * (1.0 / (total_rows * cols))
    for t in reversed(range(steps)):
        wait_back(swept.at[t], values.at[t], t)
        values[t] = values[t] - grand[t:t + 1, :]
    wait_back(mass_main, density_out, steps)
    for n in range(count):
        arrived(block(n, own).at[pl.ds(0, tiles - 1)], tile_send.at[n])
    for copy in sent:
        copy.wait_send()


def finish(values, density, values_out, density_out, sems):
    copies = [
        pltpu.make_async_copy(values, values_out, sems.at[0]),
        pltpu.make_async_copy(density, density_out, sems.at[1]),
    ]
    for copy in copies:
        copy.start()
    for copy in copies:
        copy.wait()


def per_device(pops, tiles, weights, terminal, density_history, density_init):
    _, steps, rows, cols = density_history.shape
    width = cols // tiles
    groups = steps // WINDOWS
    items = steps + groups
    outer = pops // 4
    total_rows = tiles * rows
    full = width + LANES
    dma = pltpu.SemaphoreType.DMA
    lines = max(outer - 1, 1)
    vmem = pl.BlockSpec(memory_space=pltpu.VMEM)
    anywhere = pl.BlockSpec(memory_space=pl.ANY)
    values, density = pl.pallas_call(
        functools.partial(kernel, pops, tiles),
        out_shape=(
            pltpu.VMEM((steps, rows, cols), jnp.float32),
            pltpu.VMEM((rows, cols), jnp.float32),
        ),
        in_specs=[pl.BlockSpec(memory_space=pltpu.SMEM), anywhere, anywhere, anywhere],
        out_specs=(vmem, vmem),
        scratch_shapes=[
            pltpu.VMEM((rows, cols), jnp.float32),
            pltpu.VMEM((steps, rows, cols), jnp.bfloat16),
            pltpu.VMEM((rows, cols), jnp.float32),
            dma((3,)),
            pltpu.VMEM((pops, steps, tiles, rows, width), jnp.bfloat16),
            pltpu.VMEM((pops, groups, tiles, rows, LANES), jnp.bfloat16),
            pltpu.VMEM((tiles, rows, width), jnp.float32),
            pltpu.VMEM((tiles, rows, width), jnp.float32),
            pltpu.VMEM((tiles, rows, LANES), jnp.float32),
            pltpu.VMEM((tiles, groups, rows, LANES), jnp.bfloat16),
            pltpu.VMEM((tiles, rows, LANES), jnp.float32),
            pltpu.VMEM((steps, tiles, rows, width), jnp.float32),
            pltpu.VMEM((tiles, rows, width), jnp.float32),
            pltpu.VMEM((steps, total_rows, full), jnp.float32),
            pltpu.VMEM((steps, total_rows, full), jnp.float32),
            pltpu.VMEM((steps, LANES), jnp.float32),
            pltpu.VMEM((tiles, steps, LANES), jnp.float32),
            dma((items,)), dma((items,)), dma((items,)),
            dma((3,)), dma((3,)), dma((3,)),
            dma((items,)), dma((items,)),
            dma((lines, items)), dma((lines, items)),
            dma((lines, items)), dma((lines, items)),
            dma((lines, items)), dma((lines, items)),
            dma((2 * outer, items)), dma((2 * outer, items)),
            dma((steps + 2,)), dma((steps + 2,)), dma((steps + 1,)),
        ],
        compiler_params=pltpu.CompilerParams(collective_id=0, has_side_effects=True),
    )(weights, terminal[0], density_history[0], density_init[0])
    values, density = pl.pallas_call(
        finish,
        out_shape=(
            jax.ShapeDtypeStruct((steps, rows, cols), jnp.float32),
            jax.ShapeDtypeStruct((rows, cols), jnp.float32),
        ),
        in_specs=[anywhere, anywhere],
        out_specs=(anywhere, anywhere),
        scratch_shapes=[dma((2,))],
        compiler_params=pltpu.CompilerParams(vmem_limit_bytes=8 * 1024 * 1024),
    )(values, density)
    return values[None], density[None]


def solution(mesh):
    in_specs = (P(), P("pop", "tile", None), P("pop", None, "tile", None), P("pop", "tile", None))
    out_specs = (P("pop", None, "tile", None), P("pop", "tile", None))
    body = functools.partial(per_device, mesh.shape["pop"], mesh.shape["tile"])
    return jax.shard_map(body, mesh=mesh, in_specs=in_specs, out_specs=out_specs, check_vma=False)
```
